32 devices in a mesh: dp: 4 (over y, x), tensor: 8 (over z, core).
Axes of the slice: x: 2, y: 2, z: 4, core: 2. Of those that a mesh axis runs over, the one named last changes fastest.
Arguments:
- tokens: bfloat16 [2048, 2048], P(('dp', 'tensor')), may hold values from -12 to 12
- targets: bfloat16 [2048, 2048], P(('dp', 'tensor')), may hold values from -6 to 6
- learner_gain: float32 [2048], replicated, may hold values from 0.1 to 1.9
- learner_gate: bfloat16 [2048, 8192], P(None, 'tensor'), may hold values from -0.125 to 0.125
- learner_up: bfloat16 [2048, 8192], P(None, 'tensor'), may hold values from -0.125 to 0.125
- learner_down: bfloat16 [8192, 2048], P('tensor'), may hold values from -0.0625 to 0.0625
- frozen_gain: float32 [2048], replicated, may hold values from 0.1 to 1.9
- frozen_gate: bfloat16 [2048, 8192], P(None, 'tensor'), may hold values from -0.125 to 0.125
- frozen_up: bfloat16 [2048, 8192], P(None, 'tensor'), may hold values from -0.125 to 0.125
- frozen_down: bfloat16 [8192, 2048], P('tensor'), may hold values from -0.0625 to 0.0625
Outputs:
- scores: float32 [2048], P(('dp', 'tensor'))
- grad_tokens: bfloat16 [2048, 2048], P(('dp', 'tensor'))
- grad_gain: float32 [2048], replicated
- grad_gate: float32 [2048, 8192], P('dp', 'tensor')
- grad_up: float32 [2048, 8192], P('dp', 'tensor')
- grad_down: float32 [8192, 2048], P('tensor', 'dp')
The draws below stay inside these ranges and needn't reach their ends.
All inputs are finite; a program needn't handle non-finite values.
Results may differ from the reference program's by a relative error of at most 0.0096.
Values may be sent and summed in bfloat16 or wider, within the bound.
No kernel may reach another device: no remote copies, remote signals or barrier semaphores. Data moves between devices by JAX's collectives and lax.ppermute only.
A program may use at most 128 MiB of HBM per device.

```python
import math
import jax
import jax.numpy as jnp
from jax import lax

D = 2048
FF = 8192
TOKENS = 2048


def draw_tokens(key, part):
    first, second = jax.random.split(jax.random.fold_in(key, 11))
    base = jnp.clip(jax.random.normal(first, (TOKENS, D), jnp.float32), -4.0, 4.0)
    scale = jnp.exp(jax.random.uniform(second, (TOKENS, 1), jnp.float32, math.log(0.3), math.log(3.0)))
    return (base * scale).astype(jnp.bfloat16)


def level_of(rng, dims, pieces, least, largest):
    loudness = 1.0
    for position, shards_of in pieces:
        steps = jax.random.uniform(jax.random.fold_in(jax.random.fold_in(rng, 6), position), (shards_of,), jnp.float32, least / len(pieces), largest / len(pieces))
        loudness = loudness * jnp.repeat(jnp.exp(steps), dims[position] // shards_of).reshape((-1,) + (1,) * (len(dims) - 1 - position))
    return loudness


def noise(own_key, shape, deviation, most, shards=(), held_as=jnp.bfloat16):
    values = jax.random.normal(own_key, shape, jnp.float32) * deviation
    if len(shards) > 0:
        values = level_of(own_key, shape, shards, -0.22, 0.18) * values
    return jnp.clip(values, min=-most, max=most).astype(held_as)


def setup_inputs(seed: int = 0) -> dict:
    splits = jax.random.split(jax.random.key(seed), 11)
    return {
        "tokens": draw_tokens(jax.random.fold_in(splits[10], 71), 0),
        "targets": noise(splits[1], (TOKENS, D), 1.0, 6.0, ((0, 32),)),
        "learner_gain": jnp.clip(1.0 + 0.18 * jax.random.normal(splits[2], (D,), jnp.float32), 0.1, 1.9),
        "learner_gate": noise(splits[3], (D, FF), D ** -0.5, 0.125, ((1, 8),)),
        "learner_up": noise(splits[4], (D, FF), D ** -0.5, 0.125, ((1, 8),)),
        "learner_down": noise(splits[5], (FF, D), FF ** -0.5, 0.0625, ((0, 8),)),
        "frozen_gain": jnp.clip(1.0 + 0.18 * jax.random.normal(splits[6], (D,), jnp.float32), 0.1, 1.9),
        "frozen_gate": noise(splits[7], (D, FF), D ** -0.5, 0.125, ((1, 8),)),
        "frozen_up": noise(splits[8], (D, FF), D ** -0.5, 0.125, ((1, 8),)),
        "frozen_down": noise(splits[9], (FF, D), FF ** -0.5, 0.0625, ((0, 8),)),
    }


def feed_forward(normed, w_gate, w_up, w_down):
    gate_pre = jnp.dot(normed, w_gate, preferred_element_type=jnp.float32)
    up_pre = jnp.dot(normed, w_up, preferred_element_type=jnp.float32)
    hidden = (jax.nn.silu(gate_pre) * up_pre).astype(jnp.bfloat16)
    output = jnp.dot(hidden, w_down, preferred_element_type=jnp.float32)
    return (gate_pre, up_pre, hidden, output)

def reference(tokens, targets, learner_gain, learner_gate, learner_up, learner_down, frozen_gain, frozen_gate, frozen_up, frozen_down):
    xfloat = tokens.astype(jnp.float32)
    inv_rms = lax.rsqrt(lax.optimization_barrier(jnp.mean(xfloat * xfloat, axis=-1, keepdims=True)) + 1e-05)
    normed = (xfloat * inv_rms * learner_gain).astype(jnp.bfloat16)
    frozen_normed = (xfloat * inv_rms * frozen_gain).astype(jnp.bfloat16)
    gate_pre, up_pre, hidden, learned = feed_forward(normed, learner_gate, learner_up, learner_down)
    frozen_out = feed_forward(frozen_normed, frozen_gate, frozen_up, frozen_down)[3]
    goal = targets.astype(jnp.float32)
    root = math.sqrt(tokens.shape[1])
    miss = learned - goal
    frozen_miss = frozen_out - goal
    learner_loss = 0.5 * lax.optimization_barrier(jnp.sum(miss * miss, axis=-1)) / root
    frozen_loss = 0.5 * lax.optimization_barrier(jnp.sum(frozen_miss * frozen_miss, axis=-1)) / root
    scores = learner_loss - frozen_loss
    weight = jax.nn.sigmoid(scores)
    out_grad = (weight[:, None] * miss / root).astype(jnp.bfloat16)
    grad_down = jnp.dot(hidden.T, out_grad, preferred_element_type=jnp.float32)
    hidden_grad = jnp.dot(out_grad, learner_down.T, preferred_element_type=jnp.float32)
    sigma = jax.nn.sigmoid(gate_pre)
    gate_grad = (hidden_grad * up_pre * sigma * (1.0 + gate_pre * (1.0 - sigma))).astype(jnp.bfloat16)
    up_grad = (hidden_grad * gate_pre * sigma).astype(jnp.bfloat16)
    grad_gate = jnp.dot(normed.T, gate_grad, preferred_element_type=jnp.float32)
    grad_up = jnp.dot(normed.T, up_grad, preferred_element_type=jnp.float32)
    normed_grad = jnp.dot(gate_grad, learner_gate.T, preferred_element_type=jnp.float32) + jnp.dot(up_grad, learner_up.T, preferred_element_type=jnp.float32)
    grad_gain = lax.optimization_barrier(jnp.sum(normed_grad * xfloat * inv_rms, axis=0))
    scaled = learner_gain * normed_grad
    cubed = inv_rms * inv_rms * inv_rms
    grad_tokens = (inv_rms * scaled - xfloat * cubed * lax.optimization_barrier(jnp.mean(scaled * xfloat, axis=-1, keepdims=True))).astype(jnp.bfloat16)
    return (scores, grad_tokens, grad_gain, grad_gate, grad_up, grad_down)
```

```python
import math

import jax
import jax.numpy as jnp
from jax import lax
from jax.sharding import PartitionSpec as P

BF16 = jnp.bfloat16
F32 = jnp.float32


class Ring:
    def __init__(self, size):
        self.cores = 2 if size % 2 == 0 else 1
        self.nz = size // self.cores
        self.size = size

    def swap(self, x):
        return lax.ppermute(x, "tensor", [(i, i ^ 1) for i in range(self.size)])

    def shift(self, x, k):
        step = k * self.cores
        return lax.ppermute(x, "tensor", [(i, (i + step) % self.size) for i in range(self.size)])

    def gather(self, x):
        rows = x.shape[0]
        right, left, blocks = x, x, [x]
        for d in range(1, self.nz // 2 + 1):
            if 2 * d == self.nz:
                top = self.shift(right[: rows // 2], 1)
                bottom = self.shift(left[rows // 2 :], -1)
                blocks.append(jnp.concatenate([top, bottom], axis=0))
            else:
                right, left = self.shift(right, 1), self.shift(left, -1)
                blocks += [right, left]
        if self.cores == 1:
            return blocks
        out = []
        for b in blocks:
            out += [b, self.swap(b)]
        return out

    def scatter_sum(self, p):
        rows = p.shape[1]
        p = p.reshape((self.nz, self.cores) + p.shape[1:])
        q = p[:, 0]
        if self.cores == 2:
            q = q + self.swap(p[:, 1].astype(BF16)).astype(F32)
        dist = {0: 0}
        at = 1
        for d in range(1, self.nz // 2 + 1):
            dist[-d] = at
            dist[d] = at if 2 * d == self.nz else at + 1
            at = dist[d] + 1
        total = q[0]
        half = self.nz // 2
        if half == 0:
            return total
        top = q[dist[half]][: rows // 2]
        bottom = q[dist[half]][rows // 2 :]
        right = left = None
        if self.nz % 2 == 0:
            right, left = top, bottom
        for d in range(half - 1, 0, -1):
            r_in = self.shift(right.astype(BF16), 1).astype(F32)
            l_in = self.shift(left.astype(BF16), -1).astype(F32)
            if d == half - 1:
                zeros = jnp.zeros_like(r_in)
                r_in = jnp.concatenate([r_in, zeros], axis=0)
                l_in = jnp.concatenate([zeros, l_in], axis=0)
            right, left = q[dist[d]] + r_in, q[dist[-d]] + l_in
        r_in = self.shift(right.astype(BF16), 1).astype(F32)
        l_in = self.shift(left.astype(BF16), -1).astype(F32)
        if half == 1:
            return total + jnp.concatenate([r_in, l_in], axis=0)
        return total + r_in + l_in


class Grid:
    def __init__(self, size):
        self.a = 2 if size % 2 == 0 else 1
        self.b = size // self.a
        self.size = size

    def perm(self, x, da, db):
        a, b = self.a, self.b
        if da % a == 0 and db % b == 0:
            return x
        pairs = [
            (i * b + j, ((i + da) % a) * b + (j + db) % b) for i in range(a) for j in range(b)
        ]
        return lax.ppermute(x, "dp", pairs)


def everyone_sum(x, dp, tensor):
    for axis, size in (("tensor", tensor), ("dp", dp)):
        step = 1
        while step < size:
            x = x + lax.ppermute(x, axis, [(i, i ^ step) for i in range(size)])
            step *= 2
    return x


def project_up(normed, w_gate, w_up, w_down):
    gate_pre = jnp.dot(normed, w_gate, preferred_element_type=F32)
    up_pre = jnp.dot(normed, w_up, preferred_element_type=F32)
    hidden = (jax.nn.silu(gate_pre) * up_pre).astype(BF16)
    partial_out = jnp.dot(hidden, w_down, preferred_element_type=F32)
    return (gate_pre, up_pre, hidden, partial_out)


def tdot(x, y):
    return lax.dot_general(x, y, (((0,), (0,)), ((), ())), preferred_element_type=F32)


def make_local(dp, tensor):
    ring, grid = Ring(tensor), Grid(dp)
    a, b = grid.a, grid.b

    def own_core(x):
        return x.reshape((ring.nz, ring.cores, -1) + x.shape[1:])[:, 0].reshape((-1,) + x.shape[1:])

    def both_cores(x):
        if ring.cores == 1:
            return x
        mine = x.reshape((ring.nz, 1, -1) + x.shape[1:])
        other = ring.swap(x).reshape(mine.shape)
        return jnp.concatenate([mine, other], axis=1).reshape((-1,) + x.shape[1:])

    def local(
        tokens,
        targets,
        learner_gain,
        learner_gate,
        learner_up,
        learner_down,
        frozen_gain,
        frozen_gate,
        frozen_up,
        frozen_down,
    ):
        rows, width = tokens.shape
        cols = width // dp
        me = lax.axis_index("dp")
        ya, xb = me // b, me % b

        tokens_all = jnp.concatenate(ring.gather(tokens), axis=0)
        xall = tokens_all.astype(F32)
        inv_all = lax.rsqrt(jnp.mean(xall * xall, axis=-1, keepdims=True) + 1e-05)
        normed_all = (xall * inv_all * learner_gain).astype(BF16)
        frozen_all = (xall * inv_all * frozen_gain).astype(BF16)

        gate_pre, up_pre, hidden, partial_learned = project_up(
            normed_all, learner_gate, learner_up, learner_down
        )
        learned = ring.scatter_sum(partial_learned.reshape(-1, rows, width))
        frozen_partial = project_up(frozen_all, frozen_gate, frozen_up, frozen_down)[3]
        frozen_out = ring.scatter_sum(frozen_partial.reshape(-1, rows, width))

        def columns(x, ia, ib):
            return lax.dynamic_slice_in_dim(x, (ia * b + ib) * cols, cols, axis=1)

        half_normed = own_core(normed_all)
        fast_normed, slow_normed = [], []
        for s in range(b):
            src = normed_all if s == 0 else half_normed
            piece = jnp.concatenate(
                [columns(src, (ya + r) % a, (xb + s) % b) for r in range(a)], axis=1
            )
            fast_normed.append(piece if s == 0 else both_cores(grid.perm(piece, 0, s)))
        for s in range(a):
            src = normed_all if s == 0 else half_normed
            piece = jnp.concatenate(
                [columns(src, (ya + s) % a, (xb + r) % b) for r in range(b)], axis=1
            )
            slow_normed.append(piece if s == 0 else both_cores(grid.perm(piece, s, 0)))

        mid = hidden.shape[0] // 2
        top = [grid.perm(hidden[:mid], 0, s) for s in range(b)]
        top = {(r, s): grid.perm(top[s], r, 0) for s in range(b) for r in range(a)}
        bottom = [grid.perm(hidden[mid:], r, 0) for r in range(a)]
        bottom = {(r, s): grid.perm(bottom[r], 0, s) for s in range(b) for r in range(a)}

        goal = targets.astype(F32)
        root = math.sqrt(width)
        miss = learned - goal
        frozen_miss = frozen_out - goal
        learner_loss = 0.5 * jnp.sum(miss * miss, axis=-1) / root
        frozen_loss = 0.5 * jnp.sum(frozen_miss * frozen_miss, axis=-1) / root
        scores = learner_loss - frozen_loss
        weight = jax.nn.sigmoid(scores)
        out_grad = (weight[:, None] * miss / root).astype(BF16)
        grads_all = jnp.concatenate(ring.gather(out_grad), axis=0)

        hidden_grad = jnp.dot(grads_all, learner_down.T, preferred_element_type=F32)
        sigma = jax.nn.sigmoid(gate_pre)
        gate_grad = (hidden_grad * up_pre * sigma * (1.0 + gate_pre * (1.0 - sigma))).astype(BF16)
        up_grad = (hidden_grad * gate_pre * sigma).astype(BF16)

        half_grads = own_core(grads_all)
        grad_cols = {}
        for r in range(a):
            for s in range(b):
                if r == 0 and s == 0:
                    grad_cols[r, s] = columns(grads_all, ya, xb)
                else:
                    piece = columns(half_grads, (ya + r) % a, (xb + s) % b)
                    grad_cols[r, s] = both_cores(grid.perm(piece, r, s))

        gate_parts = [grid.perm(gate_grad, 0, s) for s in range(b)]
        up_parts = [grid.perm(up_grad, s, 0) for s in range(a)]

        partial_normed = jnp.dot(
            gate_grad, learner_gate.T, preferred_element_type=F32
        ) + jnp.dot(up_grad, learner_up.T, preferred_element_type=F32)
        normed_grad = ring.scatter_sum(partial_normed.reshape(-1, rows, width))

        hidden_set = jnp.concatenate(
            [h for key in grad_cols for h in (top[key], bottom[key])], axis=0
        )
        cols_set = jnp.concatenate([grad_cols[key] for key in grad_cols], axis=0)
        grad_down = tdot(hidden_set, cols_set)

        def outer(normed_parts, grad_parts, r):
            span = slice(r * cols, (r + 1) * cols)
            return sum(tdot(n[:, span], g) for n, g in zip(normed_parts, grad_parts))

        grad_gate = outer(fast_normed, gate_parts, 0)
        for r in range(1, a):
            term = outer(fast_normed, gate_parts, r).astype(BF16)
            grad_gate = grad_gate + grid.perm(term, r, 0).astype(F32)
        grad_up = outer(slow_normed, up_parts, 0)
        for r in range(1, b):
            term = outer(slow_normed, up_parts, r).astype(BF16)
            grad_up = grad_up + grid.perm(term, 0, r).astype(F32)

        xfloat = tokens.astype(F32)
        inv_rms = lax.rsqrt(jnp.mean(xfloat * xfloat, axis=-1, keepdims=True) + 1e-05)
        gain_term = jnp.sum(normed_grad * xfloat * inv_rms, axis=0)
        grad_gain = everyone_sum(gain_term, dp, tensor)
        scaled = learner_gain * normed_grad
        cubed = inv_rms * inv_rms * inv_rms
        grad_tokens = (
            inv_rms * scaled - xfloat * cubed * jnp.mean(scaled * xfloat, axis=-1, keepdims=True)
        ).astype(BF16)
        return (scores, grad_tokens, grad_gain, grad_gate, grad_up, grad_down)

    return local


def solution(mesh):
    placed = (
        P(("dp", "tensor"), None),
        P(("dp", "tensor"), None),
        P(),
        P(None, "tensor"),
        P(None, "tensor"),
        P("tensor", None),
        P(),
        P(None, "tensor"),
        P(None, "tensor"),
        P("tensor", None),
    )
    return jax.shard_map(
        make_local(mesh.shape["dp"], mesh.shape["tensor"]),
        mesh=mesh,
        in_specs=placed,
        out_specs=(
            P(("dp", "tensor")),
            P(("dp", "tensor"), None),
            P(),
            P("dp", "tensor"),
            P("dp", "tensor"),
            P("tensor", "dp"),
        ),
        check_vma=False,
    )
```
